32 devices in a mesh: wide: 2 (over x), narrow: 4 (over y, core), depth: 4 (over z).
Axes of the slice: x: 2, y: 2, z: 4, core: 2. Of those that a mesh axis runs over, the one named last changes fastest.
Arguments:
- patch_store: bfloat16 [8, 1024, 4096], P('wide', 'depth'), may hold values from -6 to 6
- w_key: bfloat16 [4096, 1024], P(None, 'narrow'), may hold values from -0.09375 to 0.09375
- w_value: bfloat16 [4096, 1024], P(None, 'narrow'), may hold values from -0.09375 to 0.09375
- key_gain: float32 [128], replicated, may hold values from 0.1 to 1.9
- query_gain: float32 [128], replicated, may hold values from 0.1 to 1.9
- queries: bfloat16 [32, 4096], P('wide', 'narrow'), may hold values from -6 to 6
- owner_table: int32 [8], replicated, may hold values from 0 to 7, each once
- reader_table: int32 [2, 2], replicated, may hold values from 0 to 7
- request_image: int32 [32], P('wide'), may hold values from 0 to 1
- image_tiles: int32 [8], replicated, may hold values from 1 to 4
Outputs:
- context: bfloat16 [32, 4096], P(('wide', 'depth'), 'narrow')
The draws below stay inside these ranges and needn't reach their ends.
Inputs may be any that keep to these rules, and one draw needn't show every extreme that they name: owner_table is a permutation of the slots. `reader_table`: entries are image ids; a group's list may repeat an image.
All inputs are finite; a program needn't handle non-finite values.
Results may differ from the reference program's by a relative error of at most 0.012.
Values may be sent and summed in bfloat16 or wider, within the bound.
A program may use at most 64 MiB of HBM per device.

```python
import math
import jax
import jax.numpy as jnp
import numpy as np
from jax import lax

D = 4096
HEADS = 32
KV_HEADS = 8
HD = 128
TILES = 4
TILE_P = 256
READS = 2
PATCHES = 1024
IMAGES = 8
GROUPS = 2
BATCH = 32
N_WIDE = 2


def touch_ends(values, own_key, smallest, largest):
    place = [jax.random.randint(jax.random.fold_in(own_key, axis), (), 0, length) for axis, length in enumerate(values.shape)]
    main_axis = values.shape.index(max(values.shape))
    neighbour = place[:main_axis] + [(place[main_axis] + 1) % values.shape[main_axis]] + place[main_axis + 1:]
    return values.at[tuple(place)].set(smallest).at[tuple(neighbour)].set(largest)


def shard_levels(own_key, extent, split, smallest, high):
    def one(position, parts):
        heights = jax.random.uniform(jax.random.fold_in(jax.random.fold_in(own_key, 6), position), (parts,), jnp.float32, smallest / len(split), high / len(split))
        return jnp.repeat(jnp.exp(heights), extent[position] // parts).reshape((-1,) + (1,) * (len(extent) - position - 1))

    factor_of = one(*split[0])
    for cut in split[1:]:
        factor_of = factor_of * one(*cut)
    return factor_of


def rank_table(count, slope):
    portions = [(1 << 20) // math.isqrt(rank ** slope) + 1 for rank in range(1, count + 1)]
    spread = 1 + sum(portions) // (1 << 30)
    return np.cumsum(np.array([max(1, weight // spread) for weight in portions]))


def ranked_ids(key, extent, number_of, skew):
    table = rank_table(number_of, skew)
    lot = jax.random.randint(jax.random.fold_in(key, 1), extent, 0, int(table[number_of - 1]))
    standing = jnp.searchsorted(jnp.asarray(table, jnp.int32), lot, side="right")
    return jax.random.permutation(jax.random.fold_in(key, 2), number_of)[standing].astype(jnp.int32)


def centred(stream_key, shape, spread, reach, split=(), held_as=jnp.bfloat16):
    factor_of = shard_levels(stream_key, shape, split, -0.22, 0.18) if split else 1.0
    drawn = jax.random.normal(stream_key, shape, jnp.float32) * spread * factor_of
    return jnp.minimum(jnp.maximum(drawn, -reach), reach).astype(held_as)


def setup_inputs(seed: int = 0) -> dict:
    streams_of = jax.random.split(jax.random.key(seed), 11)
    return {
        "patch_store": centred(streams_of[0], (IMAGES, PATCHES, D), 1.0, 6.0, ((0, 2), (1, 4))),
        "w_key": centred(streams_of[1], (D, KV_HEADS * HD), D ** -0.5, 0.09375, ((1, 4),)),
        "w_value": centred(streams_of[2], (D, KV_HEADS * HD), D ** -0.5, 0.09375, ((1, 4),)),
        "key_gain": jnp.clip(1.0 + 0.18 * jax.random.normal(streams_of[3], (HD,), jnp.float32), 0.1, 1.9),
        "query_gain": jnp.clip(1.0 + 0.18 * jax.random.normal(streams_of[4], (HD,), jnp.float32), 0.1, 1.9),
        "queries": centred(streams_of[5], (BATCH, HEADS * HD), 1.0, 6.0, ((0, 2), (1, 4))),
        "owner_table": jax.random.permutation(streams_of[6], IMAGES).astype(jnp.int32),
        "reader_table": touch_ends(ranked_ids(streams_of[7], (GROUPS, READS), IMAGES, 1), jax.random.fold_in(streams_of[7], 3), 0, IMAGES - 1).astype(jnp.int32),
        "request_image": touch_ends(jax.random.randint(streams_of[8], (BATCH,), 0, READS), jax.random.fold_in(streams_of[8], 1), 0, READS - 1).astype(jnp.int32),
        "image_tiles": touch_ends(jax.random.randint(streams_of[9], (IMAGES,), 1, TILES + 1), jax.random.fold_in(streams_of[9], 1), 1, TILES).astype(jnp.int32),
    }


epsilon = 1e-05

def rms_scaled(tensor, scaling):
    return tensor / jnp.sqrt(lax.optimization_barrier(jnp.mean(tensor * tensor, axis=-1, keepdims=True)) + epsilon) * scaling

def reference(patch_store, w_key, w_value, key_gain, query_gain, queries, owner_table, reader_table, request_image, image_tiles):
    batch = queries.shape[0]
    per_group = batch // N_WIDE
    group_size = HEADS // KV_HEADS
    scale = 1.0 / math.sqrt(HD)

    def one_group(group_index):
        images = reader_table[group_index]
        slots = owner_table[images]
        patch_rows = patch_store[slots].reshape(READS * PATCHES, D)
        raw_keys = jnp.dot(patch_rows, w_key, preferred_element_type=jnp.float32).reshape(READS, PATCHES, KV_HEADS, HD)
        image_keys = rms_scaled(raw_keys, key_gain).astype(jnp.bfloat16)
        image_values = jnp.dot(patch_rows, w_value, preferred_element_type=jnp.float32).astype(jnp.bfloat16)
        image_values = image_values.reshape(READS, PATCHES, KV_HEADS, HD)
        first_row = (group_index * per_group).astype(jnp.int32)
        rows_here = lax.dynamic_slice_in_dim(queries, first_row, per_group, 0).astype(jnp.float32)
        normed = rms_scaled(rows_here.reshape(per_group, KV_HEADS, group_size, HD), query_gain).astype(jnp.bfloat16)
        entries = lax.dynamic_slice_in_dim(request_image, first_row, per_group, 0)
        scores = jnp.einsum('bkgd,rskd->bkgrs', normed.astype(jnp.float32), image_keys.astype(jnp.float32)) * scale
        chosen = (entries[:, None] == jnp.arange(READS, dtype=jnp.int32)[None, :]).astype(jnp.float32)
        usable = (jnp.arange(PATCHES, dtype=jnp.int32)[None, :] // TILE_P < image_tiles[images][:, None]).astype(jnp.float32)
        weights = jnp.exp(scores) * chosen[:, None, None, :, None] * usable[None, None, None]
        denominator = lax.optimization_barrier(jnp.sum(weights, axis=(3, 4)))
        numerator = jnp.einsum('bkgrs,rskd->bkgd', weights.astype(jnp.bfloat16).astype(jnp.float32), image_values.astype(jnp.float32))
        return (numerator / denominator[..., None]).astype(jnp.bfloat16).reshape(per_group, HEADS * HD)
    result = lax.map(one_group, jnp.arange(N_WIDE, dtype=jnp.int32))
    return result.reshape(batch, HEADS * HD)
```

```python
import functools
import math

import jax
import jax.numpy as jnp
from jax import lax
from jax.experimental import pallas as pl
from jax.experimental.pallas import tpu as pltpu
from jax.sharding import PartitionSpec as P

HD = 128
TILE_P = 256
EPSILON = 1e-05
MXU = 256
PIECE = 128
CHUNKS = (1, 1, 2, 4, 4, 4)
MEET = 1
MESH = pl.DeviceIdType.MESH


def kernel(
    n_wide,
    n_depth,
    store,
    w_key,
    w_value,
    key_gain,
    query_gain,
    queries,
    owner_hbm,
    reader_hbm,
    request_hbm,
    tiles_hbm,
    out,
    owner_table,
    reader_table,
    request_image,
    image_tiles,
    xbuf,
    wkbuf,
    wvbuf,
    qraw,
    gains,
    qf,
    qs,
    qx,
    row_slot,
    row_limit,
    keyed,
    valued,
    msg,
    got,
    res,
    w_sem,
    x_sem,
    q_sem,
    q_send,
    q_recv,
    m_send,
    m_recv,
):
    images, rows, width = xbuf.shape
    kv_local = wkbuf.shape[1] // HD
    batch = qraw.shape[0]
    group = qraw.shape[1] // (kv_local * HD)
    share = batch // n_depth
    block = share * group
    group_rows = n_depth * block
    peers = n_wide * n_depth
    span = PIECE // group_rows
    tiles = width // MXU
    pieces = rows // PIECE
    wide, depth = lax.axis_index("wide"), lax.axis_index("depth")
    me = wide * n_depth + depth
    part_lanes = HD // kv_local
    heads = range(kv_local)

    barrier = pltpu.get_barrier_semaphore()

    def peer(offset):
        there = {
            "wide": lax.rem(wide + offset // n_depth, n_wide),
            "depth": lax.rem(depth + offset % n_depth, n_depth),
        }
        return there["wide"] * n_depth + there["depth"], there

    small = [
        pltpu.make_async_copy(queries, qraw, q_sem.at[0]),
        pltpu.make_async_copy(query_gain, gains.at[0], q_sem.at[1]),
        pltpu.make_async_copy(key_gain, gains.at[1], q_sem.at[2]),
        pltpu.make_async_copy(owner_hbm, owner_table, q_sem.at[3]),
        pltpu.make_async_copy(reader_hbm, reader_table, q_sem.at[4]),
        pltpu.make_async_copy(request_hbm, request_image, q_sem.at[5]),
        pltpu.make_async_copy(tiles_hbm, image_tiles, q_sem.at[6]),
    ]

    starts = [sum(CHUNKS[:c]) for c in range(len(CHUNKS))]

    def chunk_copies(c):
        piece = pl.ds(starts[c] * MXU, CHUNKS[c] * MXU)
        return [
            pltpu.make_async_copy(w_key.at[piece, :], wkbuf.at[piece, :], w_sem.at[c, 0]),
            pltpu.make_async_copy(w_value.at[piece, :], wvbuf.at[piece, :], w_sem.at[c, 1]),
            pltpu.make_async_copy(store.at[:, :, piece], xbuf.at[:, :, piece], x_sem.at[c]),
        ]

    for copy in chunk_copies(0) + small:
        copy.start()
    for c in range(1, len(CHUNKS)):
        for copy in chunk_copies(c):
            copy.start()

    def greet(offset, carry):
        pl.semaphore_signal(barrier, inc=1, device_id=peer(offset)[1], device_id_type=MESH)
        return carry

    lax.fori_loop(1, peers, greet, 0, unroll=peers <= 8)

    def prepare_queries():
        gain = gains[0] * gains[1] * (1.0 / math.sqrt(HD))
        for h in range(kv_local * group):
            lanes = pl.ds(h * HD, HD)
            head = qraw[:, lanes].astype(jnp.float32)
            mean = jnp.mean(head * head, axis=-1, keepdims=True)
            qf[:, lanes] = head * lax.rsqrt(mean + EPSILON) * gain
        for k in heads:
            for t in range(n_depth):
                for g in range(group):
                    qs[pl.ds(t * block + g * share, share), :] = qf[
                        pl.ds(t * share, share), pl.ds((k * group + g) * HD, HD)
                    ]
            qx[wide, k] = qs[...].astype(jnp.bfloat16)
        row = lax.broadcasted_iota(jnp.int32, (group_rows, HD), 0)
        request = row // block * share + row % share
        entry = jnp.zeros((group_rows, HD), jnp.int32)
        for b in range(batch):
            entry = jnp.where(request == b, request_image[b], entry)
        qx[wide, kv_local] = entry.astype(jnp.float32).astype(jnp.bfloat16)

    def query_copy(offset):
        return pltpu.make_async_remote_copy(
            src_ref=qx.at[wide],
            dst_ref=qx.at[wide],
            send_sem=q_send.at[offset],
            recv_sem=q_recv.at[offset],
            device_id={"wide": lax.rem(wide + offset, n_wide)},
            device_id_type=MESH,
        )

    def query_landed(offset):
        source = lax.rem(wide + n_wide - offset, n_wide)
        return pltpu.make_async_remote_copy(
            src_ref=qx.at[source],
            dst_ref=qx.at[source],
            send_sem=q_send.at[offset],
            recv_sem=q_recv.at[offset],
            device_id={"wide": lax.rem(wide + offset, n_wide)},
            device_id_type=MESH,
        )

    def result_copy(offset):
        index, device = peer(offset)
        return pltpu.make_async_remote_copy(
            src_ref=msg.at[index],
            dst_ref=got.at[offset],
            send_sem=m_send.at[offset],
            recv_sem=m_recv.at[offset],
            device_id=device,
            device_id_type=MESH,
        )

    whole_tiles = TILE_P % rows == 0

    def read_queries():
        for offset in range(1, n_wide):
            query_landed(offset).wait_recv()
        for g in range(n_wide):
            entry = qx[g, kv_local].astype(jnp.float32)
            slots = jnp.full((group_rows, HD), -1, jnp.int32)
            limits = jnp.zeros((group_rows, HD), jnp.int32)
            for r in range(reader_table.shape[1]):
                image = reader_table[g, r]
                slot = owner_table[image]
                limit = image_tiles[image] * TILE_P - depth * rows
                if whole_tiles:
                    slot = jnp.where(limit > 0, slot, -1)
                slots = jnp.where(entry == r, slot, slots)
                limits = jnp.where(entry == r, limit, limits)
            row_slot[pl.ds(g * group_rows, group_rows), :] = slots
            row_limit[pl.ds(g * group_rows, group_rows), :] = limits

    def wider(tile):
        return jnp.concatenate([tile] * (rows // HD), axis=1) if rows > HD else tile

    def run(*flat):
        accs = [
            [flat[(k * images + j) * pieces : (k * images + j + 1) * pieces] for j in range(images)]
            for k in heads
        ]
        total = [accs[k][0][1] for k in heads]
        turn = [0]

        def next_register():
            turn[0] ^= 1
            return turn[0]

        def project(t, chosen):
            register = next_register()
            at = pl.ds(t * MXU, MXU)
            for k in heads:
                lanes = pl.ds(k * HD, HD)
                pltpu.matmul_push_rhs(
                    jnp.concatenate([wkbuf[at, lanes], wvbuf[at, lanes]], axis=1), register, k
                )
            first = True
            for j in chosen:
                for h in range(pieces):
                    patches = xbuf[j, pl.ds(h * PIECE, PIECE), at]
                    for k in heads:
                        pltpu.matmul_acc_lhs(accs[k][j][h], patches, register if first else None)
                    first = False

        def settle(k, j):
            raw = jnp.concatenate([pltpu.matmul_pop(acc) for acc in accs[k][j]], axis=0)
            head = raw[:, :HD]
            mean = jnp.mean(head * head, axis=-1, keepdims=True)
            key = (head * lax.rsqrt(mean + EPSILON)).astype(jnp.bfloat16)
            value = raw[:, HD:].astype(jnp.bfloat16)
            return jnp.concatenate([key, value], axis=1), jnp.concatenate(
                [value, jnp.ones_like(value)], axis=1
            )

        def asked(k, start):
            ask = qx[pl.ds(start, span), k].reshape(PIECE, HD)
            return jnp.concatenate([ask, jnp.zeros_like(ask)], axis=1)

        def weigh(k, j, wanted, limits):
            scores = pltpu.matmul_pop(accs[k][j][0])
            keep = wanted == wide * images + j
            if not whole_tiles:
                place = lax.broadcasted_iota(jnp.int32, keep.shape, 1)
                keep = keep & (place < limits)
            return jnp.where(keep, jnp.exp(scores), 0.0).astype(jnp.bfloat16)

        def finish(start, sums):
            dest = pl.ds(start * n_depth, span * n_depth)
            below = None
            for k in heads:
                both = sums[k].astype(jnp.bfloat16).reshape(span * n_depth, block, 2 * HD)
                msg[dest, k] = both[:, :, :HD]
                mine = sums[k][:, HD:]
                lane = lax.broadcasted_iota(jnp.int32, mine.shape, 1)
                below = mine if k == 0 else jnp.where(lane < k * part_lanes, below, mine)
            msg[dest, kv_local] = below.astype(jnp.bfloat16).reshape(span * n_depth, block, HD)

        for c in range(len(CHUNKS) - 1):
            if c == 0:
                for copy in small:
                    copy.wait()
            for copy in chunk_copies(c):
                copy.wait()
            for t in range(starts[c], starts[c] + CHUNKS[c]):
                project(t, range(images))
            if c == 0:
                prepare_queries()
            if c == MEET:
                pl.semaphore_wait(barrier, peers - 1)
                for offset in range(1, n_wide):
                    query_copy(offset).start()
        for copy in chunk_copies(len(CHUNKS) - 1):
            copy.wait()
        last = range(starts[-1], tiles)
        half = len(last) // 2
        if n_wide == span:
            read_queries()
            wanted, limits = wider(row_slot[...]), wider(row_limit[...])
            asks = [asked(k, 0) for k in heads]

            def stage_scores(j):
                register = next_register()
                for k in heads:
                    key, value = settle(k, j)
                    valued[k, j] = value
                    pltpu.matmul_push_rhs(key, register, k, transpose=True)
                    pltpu.matmul_acc_lhs(accs[k][j][0], asks[k], register)

            def stage_values(j):
                register = next_register()
                for k in heads:
                    weights = weigh(k, j, wanted, limits)
                    pltpu.matmul_push_rhs(valued[k, j], register, k)
                    pltpu.matmul_acc_lhs(total[k], weights, register)

            def stage_project(j, which):
                for t in which:
                    project(t, [j])

            for j in range(images):
                stage_project(j, last[:half])
                if j >= 2:
                    stage_values(j - 2)
                stage_project(j, last[half:])
                if j >= 1:
                    stage_scores(j - 1)
            stage_values(images - 2)
            stage_scores(images - 1)
            stage_values(images - 1)
            finish(0, [pltpu.matmul_pop(total[k]) for k in heads])
        else:
            for t in last:
                project(t, range(images))
            read_queries()
            for j in range(images):
                for k in heads:
                    keyed[k, j], valued[k, j] = settle(k, j)

            def attend(s, carry):
                start = s * span
                here = pl.ds(start * group_rows, PIECE)
                wanted, limits = wider(row_slot[here, :]), wider(row_limit[here, :])
                for j in range(images):
                    for k in heads:
                        pltpu.matmul_push_rhs(keyed[k, j], 0, k, transpose=True)
                        pltpu.matmul_acc_lhs(accs[k][j][0], asked(k, start), 0)
                for j in range(images):
                    for k in heads:
                        weights = weigh(k, j, wanted, limits)
                        pltpu.matmul_push_rhs(valued[k, j], 0, k)
                        pltpu.matmul_acc_lhs(total[k], weights, 0)
                finish(start, [pltpu.matmul_pop(total[k]) for k in heads])
                return carry

            lax.fori_loop(0, n_wide // span, attend, 0)

    pl.run_scoped(
        run,
        *[
            pltpu.ACC(k)((PIECE, MXU), jnp.float32)
            for k in heads
            for _ in range(images * pieces)
        ],
    )

    if peers <= 8:
        order = [
            a * n_depth + b
            for b in [*range(1, n_depth), 0]
            for a in [*range(1, n_wide), 0]
            if a or b
        ]
        for offset in order:
            result_copy(offset).start()
        total = msg[me].astype(jnp.float32)
        for offset in order[::-1]:
            result_copy(offset).wait_recv()
            total = total + got[offset].astype(jnp.float32)
    else:

        def step(offset, carry):
            result_copy(offset).start()
            return carry

        lax.fori_loop(1, peers, step, 0)

        def collect(offset, total):
            result_copy(offset).wait_recv()
            return total + got[offset].astype(jnp.float32)

        total = lax.fori_loop(1, peers, collect, msg[me].astype(jnp.float32))
    for k in heads:
        res[...] = total[k] / total[kv_local, :, k * part_lanes : k * part_lanes + 1]
        for g in range(group):
            out[:, pl.ds((k * group + g) * HD, HD)] = res[pl.ds(g * share, share), :].astype(
                out.dtype
            )

    for offset in range(1, n_wide):
        query_copy(offset).wait_send()

    def drain(offset, carry):
        result_copy(offset).wait_send()
        return carry

    lax.fori_loop(1, peers, drain, 0, unroll=peers <= 8)


def local(
    n_wide,
    n_depth,
    patch_store,
    w_key,
    w_value,
    key_gain,
    query_gain,
    queries,
    owner_table,
    reader_table,
    request_image,
    image_tiles,
):
    images, rows, width = patch_store.shape
    kv_local = w_key.shape[1] // HD
    batch, q_cols = queries.shape
    group = q_cols // (kv_local * HD)
    share = batch // n_depth
    block = share * group
    group_rows = n_depth * block
    peers = n_wide * n_depth
    total_rows = peers * block
    anywhere = pl.BlockSpec(memory_space=pl.ANY)
    dma = pltpu.SemaphoreType.DMA
    return pl.pallas_call(
        functools.partial(kernel, n_wide, n_depth),
        out_shape=pltpu.VMEM((share, q_cols), jnp.bfloat16),
        in_specs=[anywhere] * 10,
        out_specs=pl.BlockSpec(memory_space=pltpu.VMEM),
        scratch_shapes=[
            pltpu.SMEM(owner_table.shape, jnp.int32),
            pltpu.SMEM(reader_table.shape, jnp.int32),
            pltpu.SMEM(request_image.shape, jnp.int32),
            pltpu.SMEM(image_tiles.shape, jnp.int32),
            pltpu.VMEM((images, rows, width), jnp.bfloat16),
            pltpu.VMEM((width, kv_local * HD), jnp.bfloat16),
            pltpu.VMEM((width, kv_local * HD), jnp.bfloat16),
            pltpu.VMEM((batch, q_cols), jnp.bfloat16),
            pltpu.VMEM((2, 1, HD), jnp.float32),
            pltpu.VMEM((batch, q_cols), jnp.float32),
            pltpu.VMEM((group_rows, HD), jnp.float32),
            pltpu.VMEM((n_wide, kv_local + 1, group_rows, HD), jnp.bfloat16),
            pltpu.VMEM((total_rows, HD), jnp.int32),
            pltpu.VMEM((total_rows, HD), jnp.int32),
            pltpu.VMEM((kv_local, images, rows, 2 * HD), jnp.bfloat16),
            pltpu.VMEM((kv_local, images, rows, 2 * HD), jnp.bfloat16),
            pltpu.VMEM((peers, kv_local + 1, block, HD), jnp.bfloat16),
            pltpu.VMEM((peers, kv_local + 1, block, HD), jnp.bfloat16),
            pltpu.VMEM((block, HD), jnp.float32),
            dma((len(CHUNKS), 2)),
            dma((len(CHUNKS),)),
            dma((7,)),
            dma((n_wide,)),
            dma((n_wide,)),
            dma((peers,)),
            dma((peers,)),
        ],
        compiler_params=pltpu.CompilerParams(
            collective_id=0, has_side_effects=True, vmem_limit_bytes=56 * 1024 * 1024
        ),
    )(
        patch_store,
        w_key,
        w_value,
        key_gain.reshape(1, HD),
        query_gain.reshape(1, HD),
        queries,
        owner_table,
        reader_table,
        request_image,
        image_tiles,
    )


def solution(mesh):
    placed = (
        P("wide", "depth", None),
        P(None, "narrow"),
        P(None, "narrow"),
        P(),
        P(),
        P("wide", "narrow"),
        P(),
        P(),
        P("wide"),
        P(),
    )
    return jax.shard_map(
        functools.partial(local, mesh.shape["wide"], mesh.shape["depth"]),
        mesh=mesh,
        in_specs=placed,
        out_specs=P(("wide", "depth"), "narrow"),
        check_vma=False,
    )
```

```python
import functools
import math

import jax
import jax.numpy as jnp
from jax import lax
from jax.experimental import pallas as pl
from jax.experimental.pallas import tpu as pltpu
from jax.sharding import PartitionSpec as P

HD = 128
TILE_P = 256
EPSILON = 1e-05
MXU = 256
MXUS = 2
CHUNKS = (2, 2, 4, 4, 4)
AHEAD = 8
MEET = 0
MESH = pl.DeviceIdType.MESH


def kernel(
    n_wide,
    n_depth,
    store,
    w_key,
    w_value,
    key_gain,
    query_gain,
    queries,
    owner_hbm,
    reader_hbm,
    request_hbm,
    tiles_hbm,
    out,
    owner_table,
    reader_table,
    request_image,
    image_tiles,
    xbuf,
    wkbuf,
    wvbuf,
    qraw,
    gains,
    qf,
    qs,
    qx,
    row_slot,
    row_limit,
    keyed,
    valued,
    weighed,
    sums,
    msg,
    got,
    res,
    c_sem,
    q_sem,
    q_send,
    q_recv,
    m_send,
    m_recv,
):
    images, rows, width = xbuf.shape
    kv_local = wkbuf.shape[1] // HD
    batch = qraw.shape[0]
    group = qraw.shape[1] // (kv_local * HD)
    share = batch // n_depth
    block = share * group
    group_rows = n_depth * block
    peers = n_wide * n_depth
    asked_rows = MXU // kv_local
    span = asked_rows // group_rows
    tiles = width // MXU
    pairs = images // MXUS
    wide, depth = lax.axis_index("wide"), lax.axis_index("depth")
    me = wide * n_depth + depth
    part_lanes = HD // kv_local
    heads = range(kv_local)

    barrier = pltpu.get_barrier_semaphore()

    def peer(offset):
        there = {
            "wide": lax.rem(wide + offset // n_depth, n_wide),
            "depth": lax.rem(depth + offset % n_depth, n_depth),
        }
        return there["wide"] * n_depth + there["depth"], there

    small = [
        pltpu.make_async_copy(queries, qraw, q_sem.at[0]),
        pltpu.make_async_copy(query_gain, gains.at[0], q_sem.at[0]),
        pltpu.make_async_copy(key_gain, gains.at[1], q_sem.at[0]),
        pltpu.make_async_copy(owner_hbm, owner_table, q_sem.at[0]),
        pltpu.make_async_copy(reader_hbm, reader_table, q_sem.at[0]),
        pltpu.make_async_copy(request_hbm, request_image, q_sem.at[0]),
        pltpu.make_async_copy(tiles_hbm, image_tiles, q_sem.at[0]),
    ]

    starts = [sum(CHUNKS[:c]) for c in range(len(CHUNKS))]

    def chunk_copies(c):
        piece = pl.ds(starts[c] * MXU, CHUNKS[c] * MXU)
        return [
            [
                pltpu.make_async_copy(w_key.at[piece, :], wkbuf.at[piece, :], c_sem.at[c, 0]),
                pltpu.make_async_copy(store.at[:, :, piece], xbuf.at[:, :, piece], c_sem.at[c, 0]),
            ],
            [pltpu.make_async_copy(w_value.at[piece, :], wvbuf.at[piece, :], c_sem.at[c, 1])],
        ]

    def begin(copies):
        for copy in copies:
            copy.start()

    def end(copies):
        for copy in copies:
            copy.wait()

    begun = [0]

    def fetch(arrived):
        while begun[0] < len(CHUNKS):
            c = begun[0]
            if c and starts[c] + CHUNKS[c] > arrived + AHEAD:
                break
            keys_part, values_part = chunk_copies(c)
            begin(keys_part)
            if c == 0:
                begin(small)
            begin(values_part)
            begun[0] += 1

    fetch(0)

    def greet(offset, carry):
        pl.semaphore_signal(barrier, inc=1, device_id=peer(offset)[1], device_id_type=MESH)
        return carry

    lax.fori_loop(1, peers, greet, 0, unroll=peers <= 8)

    def prepare_queries():
        gain = gains[0] * gains[1] * (1.0 / math.sqrt(HD))
        for h in range(kv_local * group):
            lanes = pl.ds(h * HD, HD)
            head = qraw[:, lanes].astype(jnp.float32)
            mean = jnp.mean(head * head, axis=-1, keepdims=True)
            qf[:, lanes] = head * lax.rsqrt(mean + EPSILON) * gain
        for k in heads:
            for t in range(n_depth):
                for g in range(group):
                    qs[pl.ds(t * block + g * share, share), :] = qf[
                        pl.ds(t * share, share), pl.ds((k * group + g) * HD, HD)
                    ]
            qx[wide, k] = qs[...].astype(jnp.bfloat16)
        row = lax.broadcasted_iota(jnp.int32, (group_rows, HD), 0)
        request = row // block * share + row % share
        entry = jnp.zeros((group_rows, HD), jnp.int32)
        for b in range(batch):
            entry = jnp.where(request == b, request_image[b], entry)
        qx[wide, kv_local] = entry.astype(jnp.float32).astype(jnp.bfloat16)

    def query_copy(offset):
        return pltpu.make_async_remote_copy(
            src_ref=qx.at[wide],
            dst_ref=qx.at[wide],
            send_sem=q_send.at[offset - 1],
            recv_sem=q_recv.at[offset - 1],
            device_id={"wide": lax.rem(wide + offset, n_wide)},
            device_id_type=MESH,
        )

    def query_landed(offset):
        source = lax.rem(wide + n_wide - offset, n_wide)
        return pltpu.make_async_remote_copy(
            src_ref=qx.at[source],
            dst_ref=qx.at[source],
            send_sem=q_send.at[offset - 1],
            recv_sem=q_recv.at[offset - 1],
            device_id={"wide": lax.rem(wide + offset, n_wide)},
            device_id_type=MESH,
        )

    def result_copy(offset):
        index, device = peer(offset)
        return pltpu.make_async_remote_copy(
            src_ref=msg.at[index],
            dst_ref=got.at[offset - 1],
            send_sem=m_send.at[0],
            recv_sem=m_recv.at[0],
            device_id=device,
            device_id_type=MESH,
        )

    def all_results():
        every = pl.ds(0, peers - 1)
        return pltpu.make_async_remote_copy(
            src_ref=msg.at[every],
            dst_ref=got.at[every],
            send_sem=m_send.at[0],
            recv_sem=m_recv.at[0],
            device_id=peer(1)[1],
            device_id_type=MESH,
        )

    whole_tiles = TILE_P % rows == 0

    def read_queries():
        for offset in range(1, n_wide):
            query_landed(offset).wait_recv()
        for g in range(n_wide):
            entry = qx[g, kv_local].astype(jnp.float32)
            slots = jnp.full((group_rows, HD), -1, jnp.int32)
            limits = jnp.zeros((group_rows, HD), jnp.int32)
            for r in range(reader_table.shape[1]):
                image = reader_table[g, r]
                slot = owner_table[image]
                limit = image_tiles[image] * TILE_P - depth * rows
                if whole_tiles:
                    slot = jnp.where(limit > 0, slot, -1)
                slots = jnp.where(entry == r, slot, slots)
                limits = jnp.where(entry == r, limit, limits)
            row_slot[pl.ds(g * group_rows, group_rows), :] = slots
            row_limit[pl.ds(g * group_rows, group_rows), :] = limits

    def wider(tile):
        return jnp.concatenate([tile] * (rows // HD), axis=1) if rows > HD else tile

    def run(*flat):
        accs = [flat[2 * j : 2 * j + 2] for j in range(images)]
        mine = [range(m * pairs, (m + 1) * pairs) for m in range(MXUS)]
        total = [accs[mine[m][0]][0] for m in range(MXUS)]
        turn = [0]

        def next_register():
            turn[0] ^= 1
            return turn[0]

        def project(t, part, chosen):
            register = next_register()
            at = pl.ds(t * MXU, MXU)
            weight = (wkbuf, wvbuf)[part][at, :]
            for m in range(MXUS):
                pltpu.matmul_push_rhs(weight, register, m)
            first = True
            for i in chosen:
                for m in range(MXUS):
                    j = mine[m][i]
                    pltpu.matmul_acc_lhs(
                        accs[j][part], xbuf[j, :, at], register if first else None
                    )
                first = False

        def settle_keys(j):
            raw = pltpu.matmul_pop(accs[j][0])
            done = []
            for k in heads:
                head = raw[:, k * HD : (k + 1) * HD]
                mean = jnp.mean(head * head, axis=-1, keepdims=True)
                done.append((head * lax.rsqrt(mean + EPSILON)).astype(jnp.bfloat16))
            return jnp.concatenate(done, axis=1)

        def settle_values(j):
            return pltpu.matmul_pop(accs[j][1]).astype(jnp.bfloat16)

        def asked(start):
            lines = []
            for k in heads:
                ask = qx[pl.ds(start, span), k].reshape(asked_rows, HD)
                none = jnp.zeros_like(ask)
                lines.append(jnp.concatenate([ask if k == i else none for i in heads], axis=1))
            return jnp.concatenate(lines, axis=0)

        def weigh(j, wanted, limits):
            scores = pltpu.matmul_pop(accs[j][0])
            keep = wanted == wide * images + j
            if not whole_tiles:
                place = lax.broadcasted_iota(jnp.int32, keep.shape, 1)
                keep = keep & (place < limits)
            keep = jnp.concatenate([keep] * kv_local, axis=0)
            weights = jnp.where(keep, jnp.exp(scores), 0.0)
            weighed[j] = weights.astype(jnp.bfloat16)
            lanes = weights[:, :HD]
            for at in range(HD, rows, HD):
                lanes = lanes + weights[:, at : at + HD]
            return lanes

        def send_denominators(start):
            dest = pl.ds(start * n_depth, span * n_depth)
            below = jnp.sum(sums[...], axis=-1, keepdims=True)
            lane = lax.broadcasted_iota(jnp.int32, (asked_rows, HD), 1)
            plane = jnp.broadcast_to(below[:asked_rows], (asked_rows, HD))
            for k in heads[1:]:
                plane = jnp.where(
                    lane < k * part_lanes, plane, below[k * asked_rows : (k + 1) * asked_rows]
                )
            msg[dest, kv_local] = plane.astype(jnp.bfloat16).reshape(span * n_depth, block, HD)

        def finish(start):
            dest = pl.ds(start * n_depth, span * n_depth)
            both = [pltpu.matmul_pop(total[m]) for m in range(MXUS)]
            for k in heads:
                line, lanes = slice(k * asked_rows, (k + 1) * asked_rows), slice(k * HD, (k + 1) * HD)
                number = both[0][line, lanes]
                for m in range(1, MXUS):
                    number = number + both[m][line, lanes]
                msg[dest, k] = number.astype(jnp.bfloat16).reshape(span * n_depth, block, HD)

        for c in range(len(CHUNKS) - 1):
            if c == 0:
                end(small)
            for part in range(2):
                end(chunk_copies(c)[part])
                if part == 0:
                    fetch(starts[c] + CHUNKS[c])
                for t in range(starts[c], starts[c] + CHUNKS[c]):
                    project(t, part, range(pairs))
                if c == 0 and part == 0:
                    prepare_queries()
            if c == MEET:
                pl.semaphore_wait(barrier, peers - 1)
                for offset in range(1, n_wide):
                    query_copy(offset).start()
        keys_last, values_last = chunk_copies(len(CHUNKS) - 1)
        end(keys_last)
        last = range(starts[-1], tiles)
        half = len(last) // 2

        def stage_scores(i, ask):
            register = next_register()
            for m in range(MXUS):
                j = mine[m][i]
                pltpu.matmul_push_rhs(settle_keys(j), register, m, transpose=True)
                pltpu.matmul_acc_lhs(accs[j][0], ask, register)

        def stage_weights(i, wanted, limits):
            for m in range(MXUS):
                lanes = weigh(mine[m][i], wanted, limits)
                if i == 0 and m == 0:
                    sums[...] = lanes
                else:
                    sums[...] += lanes

        def stage_values(i):
            register = next_register()
            for m in range(MXUS):
                j = mine[m][i]
                pltpu.matmul_push_rhs(settle_values(j), register, m)
                pltpu.matmul_acc_lhs(total[m], weighed[j], register)

        def stage_project(i, part, which):
            for t in which:
                project(t, part, [i])

        if n_wide == span:
            read_queries()
            wanted, limits = wider(row_slot[...]), wider(row_limit[...])
            ask = asked(0)
            for i in range(pairs):
                stage_project(i, 0, last)
            end(values_last)
            for i in range(pairs):
                stage_project(i, 1, last[:half])
                if i > 0:
                    stage_weights(i - 1, wanted, limits)
                    stage_values(i - 1)
                stage_project(i, 1, last[half:]) if i + 1 < pairs else None
                stage_scores(i, ask)
                if i + 1 == pairs:
                    stage_project(i, 1, last[half:])
            stage_weights(pairs - 1, wanted, limits)
            send_denominators(0)
            stage_values(pairs - 1)
            finish(0)
        else:
            end(values_last)
            for t in last:
                for part in range(2):
                    project(t, part, range(pairs))
            read_queries()
            for j in range(images):
                keyed[j], valued[j] = settle_keys(j), settle_values(j)

            def attend(s, carry):
                start = s * span
                here = pl.ds(start * group_rows, asked_rows)
                wanted, limits = wider(row_slot[here, :]), wider(row_limit[here, :])
                ask = asked(start)
                for i in range(pairs):
                    for m in range(MXUS):
                        j = mine[m][i]
                        pltpu.matmul_push_rhs(keyed[j], 0, m, transpose=True)
                        pltpu.matmul_acc_lhs(accs[j][0], ask, 0)
                for i in range(pairs):
                    stage_weights(i, wanted, limits)
                for i in range(pairs):
                    for m in range(MXUS):
                        j = mine[m][i]
                        pltpu.matmul_push_rhs(valued[j], 0, m)
                        pltpu.matmul_acc_lhs(total[m], weighed[j], 0)
                send_denominators(start)
                finish(start)
                return carry

            lax.fori_loop(0, n_wide // span, attend, 0)

    pl.run_scoped(
        run,
        *[
            pltpu.ACC(j // pairs)((rows, MXU), jnp.float32)
            for j in range(images)
            for _ in range(2)
        ],
    )

    if peers <= 8:
        order = [
            a * n_depth + b
            for b in [*range(1, n_depth), 0]
            for a in [*range(1, n_wide), 0]
            if a or b
        ]
        for offset in order:
            result_copy(offset).start()
    else:

        def step(offset, carry):
            result_copy(offset).start()
            return carry

        lax.fori_loop(1, peers, step, 0)

    total = msg[me].astype(jnp.float32)
    all_results().wait_recv()

    def collect(offset, total):
        return total + got[offset - 1].astype(jnp.float32)

    total = lax.fori_loop(1, peers, collect, total, unroll=peers <= 8)
    for k in heads:
        res[...] = total[k] / total[kv_local, :, k * part_lanes : k * part_lanes + 1]
        for g in range(group):
            out[:, pl.ds((k * group + g) * HD, HD)] = res[pl.ds(g * share, share), :].astype(
                out.dtype
            )

    for offset in range(1, n_wide):
        query_copy(offset).wait_send()

    all_results().wait_send()


def local(
    n_wide,
    n_depth,
    patch_store,
    w_key,
    w_value,
    key_gain,
    query_gain,
    queries,
    owner_table,
    reader_table,
    request_image,
    image_tiles,
):
    images, rows, width = patch_store.shape
    kv_local = w_key.shape[1] // HD
    batch, q_cols = queries.shape
    group = q_cols // (kv_local * HD)
    share = batch // n_depth
    block = share * group
    group_rows = n_depth * block
    peers = n_wide * n_depth
    total_rows = peers * block
    anywhere = pl.BlockSpec(memory_space=pl.ANY)
    dma = pltpu.SemaphoreType.DMA
    return pl.pallas_call(
        functools.partial(kernel, n_wide, n_depth),
        out_shape=pltpu.VMEM((share, q_cols), jnp.bfloat16),
        in_specs=[anywhere] * 10,
        out_specs=pl.BlockSpec(memory_space=pltpu.VMEM),
        scratch_shapes=[
            pltpu.SMEM(owner_table.shape, jnp.int32),
            pltpu.SMEM(reader_table.shape, jnp.int32),
            pltpu.SMEM(request_image.shape, jnp.int32),
            pltpu.SMEM(image_tiles.shape, jnp.int32),
            pltpu.VMEM((images, rows, width), jnp.bfloat16),
            pltpu.VMEM((width, kv_local * HD), jnp.bfloat16),
            pltpu.VMEM((width, kv_local * HD), jnp.bfloat16),
            pltpu.VMEM((batch, q_cols), jnp.bfloat16),
            pltpu.VMEM((2, 1, HD), jnp.float32),
            pltpu.VMEM((batch, q_cols), jnp.float32),
            pltpu.VMEM((group_rows, HD), jnp.float32),
            pltpu.VMEM((n_wide, kv_local + 1, group_rows, HD), jnp.bfloat16),
            pltpu.VMEM((total_rows, HD), jnp.int32),
            pltpu.VMEM((total_rows, HD), jnp.int32),
            pltpu.VMEM((images, rows, kv_local * HD), jnp.bfloat16),
            pltpu.VMEM((images, rows, kv_local * HD), jnp.bfloat16),
            pltpu.VMEM((images, MXU, rows), jnp.bfloat16),
            pltpu.VMEM((MXU, HD), jnp.float32),
            pltpu.VMEM((peers, kv_local + 1, block, HD), jnp.bfloat16),
            pltpu.VMEM((peers - 1, kv_local + 1, block, HD), jnp.bfloat16),
            pltpu.VMEM((block, HD), jnp.float32),
            dma((len(CHUNKS), 2)),
            dma((1,)),
            dma((n_wide - 1,)),
            dma((n_wide - 1,)),
            dma((1,)),
            dma((1,)),
        ],
        compiler_params=pltpu.CompilerParams(
            collective_id=0, has_side_effects=True, vmem_limit_bytes=56 * 1024 * 1024
        ),
    )(
        patch_store,
        w_key,
        w_value,
        key_gain.reshape(1, HD),
        query_gain.reshape(1, HD),
        queries,
        owner_table,
        reader_table,
        request_image,
        image_tiles,
    )


def solution(mesh):
    placed = (
        P("wide", "depth", None),
        P(None, "narrow"),
        P(None, "narrow"),
        P(),
        P(),
        P("wide", "narrow"),
        P(),
        P(),
        P("wide"),
        P(),
    )
    return jax.shard_map(
        functools.partial(local, mesh.shape["wide"], mesh.shape["depth"]),
        mesh=mesh,
        in_specs=placed,
        out_specs=P(("wide", "depth"), "narrow"),
        check_vma=False,
    )
```

```python
import functools
import math

import jax
import jax.numpy as jnp
from jax import lax
from jax.experimental import pallas as pl
from jax.experimental.pallas import tpu as pltpu
from jax.sharding import PartitionSpec as P

HD = 128
TILE_P = 256
EPSILON = 1e-05
MXU = 256
MXUS = 2
CHUNKS = (2, 2, 4, 4, 4)
AHEAD = 8
MEET = 0
MESH = pl.DeviceIdType.MESH


def kernel(
    n_wide,
    n_depth,
    store,
    w_key,
    w_value,
    key_gain,
    query_gain,
    queries,
    owner_hbm,
    reader_hbm,
    request_hbm,
    tiles_hbm,
    out,
    owner_table,
    reader_table,
    request_image,
    image_tiles,
    xbuf,
    wkbuf,
    wvbuf,
    qraw,
    gains,
    qf,
    qs,
    qx,
    row_slot,
    row_limit,
    keyed,
    valued,
    weighed,
    sums,
    msg,
    got,
    res,
    c_sem,
    q_sem,
    q_send,
    q_recv,
    m_send,
    m_recv,
):
    images, rows, width = xbuf.shape
    kv_local = wkbuf.shape[1] // HD
    batch = qraw.shape[0]
    group = qraw.shape[1] // (kv_local * HD)
    share = batch // n_depth
    block = share * group
    group_rows = n_depth * block
    peers = n_wide * n_depth
    asked_rows = MXU // kv_local
    span = asked_rows // group_rows
    tiles = width // MXU
    pairs = images // MXUS
    wide, depth = lax.axis_index("wide"), lax.axis_index("depth")
    me = wide * n_depth + depth
    part_lanes = HD // kv_local
    heads = range(kv_local)

    barrier = pltpu.get_barrier_semaphore()

    def peer(offset):
        there = {
            "wide": lax.rem(wide + offset // n_depth, n_wide),
            "depth": lax.rem(depth + offset % n_depth, n_depth),
        }
        return there["wide"] * n_depth + there["depth"], there

    small = [
        pltpu.make_async_copy(queries, qraw, q_sem.at[0]),
        pltpu.make_async_copy(query_gain, gains.at[0], q_sem.at[0]),
        pltpu.make_async_copy(key_gain, gains.at[1], q_sem.at[0]),
        pltpu.make_async_copy(owner_hbm, owner_table, q_sem.at[0]),
        pltpu.make_async_copy(reader_hbm, reader_table, q_sem.at[0]),
        pltpu.make_async_copy(request_hbm, request_image, q_sem.at[0]),
        pltpu.make_async_copy(tiles_hbm, image_tiles, q_sem.at[0]),
    ]

    starts = [sum(CHUNKS[:c]) for c in range(len(CHUNKS))]

    final = len(CHUNKS) - 1

    def chunk_copies(c):
        piece = pl.ds(starts[c] * MXU, CHUNKS[c] * MXU)
        return [
            pltpu.make_async_copy(w_key.at[piece, :], wkbuf.at[piece, :], c_sem.at[c]),
            pltpu.make_async_copy(store.at[:, :, piece], xbuf.at[:, :, piece], c_sem.at[c]),
            pltpu.make_async_copy(
                w_value.at[piece, :], wvbuf.at[piece, :], c_sem.at[c]
            ),
        ]

    def begin(copies):
        for copy in copies:
            copy.start()

    def end(copies):
        for copy in copies:
            copy.wait()

    begun = [0]

    def fetch(arrived):
        while begun[0] < len(CHUNKS):
            c = begun[0]
            if c and starts[c] + CHUNKS[c] > arrived + AHEAD:
                break
            begin(chunk_copies(c))
            if c == 0:
                begin(small)
            begun[0] += 1

    fetch(0)

    def greet(offset, carry):
        pl.semaphore_signal(barrier, inc=1, device_id=peer(offset)[1], device_id_type=MESH)
        return carry

    lax.fori_loop(1, peers, greet, 0, unroll=peers <= 8)

    def prepare_queries():
        gain = gains[0] * gains[1] * (1.0 / math.sqrt(HD))
        for h in range(kv_local * group):
            lanes = pl.ds(h * HD, HD)
            head = qraw[:, lanes].astype(jnp.float32)
            mean = jnp.mean(head * head, axis=-1, keepdims=True)
            qf[:, lanes] = head * lax.rsqrt(mean + EPSILON) * gain
        for k in heads:
            for t in range(n_depth):
                for g in range(group):
                    qs[pl.ds(t * block + g * share, share), :] = qf[
                        pl.ds(t * share, share), pl.ds((k * group + g) * HD, HD)
                    ]
            qx[wide, k] = qs[...].astype(jnp.bfloat16)
        row = lax.broadcasted_iota(jnp.int32, (group_rows, HD), 0)
        request = row // block * share + row % share
        entry = jnp.zeros((group_rows, HD), jnp.int32)
        for b in range(batch):
            entry = jnp.where(request == b, request_image[b], entry)
        qx[wide, kv_local] = entry.astype(jnp.float32).astype(jnp.bfloat16)

    def query_copy(offset):
        return pltpu.make_async_remote_copy(
            src_ref=qx.at[wide],
            dst_ref=qx.at[wide],
            send_sem=q_send.at[offset - 1],
            recv_sem=q_recv.at[offset - 1],
            device_id={"wide": lax.rem(wide + offset, n_wide)},
            device_id_type=MESH,
        )

    def query_landed(offset):
        source = lax.rem(wide + n_wide - offset, n_wide)
        return pltpu.make_async_remote_copy(
            src_ref=qx.at[source],
            dst_ref=qx.at[source],
            send_sem=q_send.at[offset - 1],
            recv_sem=q_recv.at[offset - 1],
            device_id={"wide": lax.rem(wide + offset, n_wide)},
            device_id_type=MESH,
        )

    def result_copy(offset):
        index, device = peer(offset)
        return pltpu.make_async_remote_copy(
            src_ref=msg.at[index],
            dst_ref=got.at[offset - 1],
            send_sem=m_send.at[0],
            recv_sem=m_recv.at[0],
            device_id=device,
            device_id_type=MESH,
        )

    def all_results():
        every = pl.ds(0, peers - 1)
        return pltpu.make_async_remote_copy(
            src_ref=msg.at[every],
            dst_ref=got.at[every],
            send_sem=m_send.at[0],
            recv_sem=m_recv.at[0],
            device_id=peer(1)[1],
            device_id_type=MESH,
        )

    whole_tiles = TILE_P % rows == 0

    def read_queries():
        for offset in range(1, n_wide):
            query_landed(offset).wait_recv()
        for g in range(n_wide):
            entry = qx[g, kv_local].astype(jnp.float32)
            slots = jnp.full((group_rows, HD), -1, jnp.int32)
            limits = jnp.zeros((group_rows, HD), jnp.int32)
            for r in range(reader_table.shape[1]):
                image = reader_table[g, r]
                slot = owner_table[image]
                limit = image_tiles[image] * TILE_P - depth * rows
                if whole_tiles:
                    slot = jnp.where(limit > 0, slot, -1)
                slots = jnp.where(entry == r, slot, slots)
                limits = jnp.where(entry == r, limit, limits)
            row_slot[pl.ds(g * group_rows, group_rows), :] = slots
            row_limit[pl.ds(g * group_rows, group_rows), :] = limits

    def wider(tile):
        return jnp.concatenate([tile] * (rows // HD), axis=1) if rows > HD else tile

    def run(*flat):
        accs = [flat[MXUS * j : MXUS * (j + 1)] for j in range(images)]
        total = [accs[0][0], accs[pairs][1]]
        turn = [0] * MXUS
        ready = []

        def push(tile, m, transpose=False):
            turn[m] ^= 1
            pltpu.matmul_push_rhs(tile, turn[m], m, transpose=transpose)
            return turn[m]

        def push_weights(step):
            ready.append(
                [
                    push((wkbuf, wvbuf)[part][pl.ds(t * MXU, MXU), :], m)
                    for m, (part, t) in enumerate(step[0])
                ]
            )

        def project(steps, after=None):
            if not ready:
                push_weights(steps[0])
            for n, (weights, rounds) in enumerate(steps):
                registers = ready.pop()
                for first, (j, slots) in enumerate(rounds):
                    patches = {}
                    for m, (part, t) in enumerate(weights):
                        if t not in patches:
                            patches[t] = xbuf[j, :, pl.ds(t * MXU, MXU)]
                        pltpu.matmul_acc_lhs(
                            slots[m], patches[t], None if first else registers[m]
                        )
                following = steps[n + 1] if n + 1 < len(steps) else after
                if following:
                    push_weights(following)

        def together(t, chosen):
            return [(0, t), (1, t)], [(j, accs[j]) for j in chosen]

        def apart(part, j, t, u):
            slots = [accs[j][0], accs[j - pairs if part == 0 else j][1]]
            return [(part, t), (part, u)], [(j, slots)]

        def popped(slots):
            return functools.reduce(jnp.add, [pltpu.matmul_pop(slot) for slot in slots])

        def settle_keys(slots):
            raw = popped(slots)
            done = []
            for k in heads:
                head = raw[:, k * HD : (k + 1) * HD]
                mean = jnp.mean(head * head, axis=-1, keepdims=True)
                done.append((head * lax.rsqrt(mean + EPSILON)).astype(jnp.bfloat16))
            return jnp.concatenate(done, axis=1)

        def settle_values(slots):
            return popped(slots).astype(jnp.bfloat16)

        def asked(start):
            lines = []
            for k in heads:
                ask = qx[pl.ds(start, span), k].reshape(asked_rows, HD)
                none = jnp.zeros_like(ask)
                lines.append(jnp.concatenate([ask if k == i else none for i in heads], axis=1))
            return jnp.concatenate(lines, axis=0)

        def weigh(j, slot, wanted, limits):
            scores = pltpu.matmul_pop(slot)
            keep = wanted == wide * images + j
            if not whole_tiles:
                place = lax.broadcasted_iota(jnp.int32, keep.shape, 1)
                keep = keep & (place < limits)
            keep = jnp.concatenate([keep] * kv_local, axis=0)
            weights = jnp.where(keep, jnp.exp(scores), 0.0)
            weighed[j] = weights.astype(jnp.bfloat16)
            lanes = weights[:, :HD]
            for at in range(HD, rows, HD):
                lanes = lanes + weights[:, at : at + HD]
            return lanes

        def send_denominators(start):
            dest = pl.ds(start * n_depth, span * n_depth)
            below = jnp.sum(sums[...], axis=-1, keepdims=True)
            lane = lax.broadcasted_iota(jnp.int32, (asked_rows, HD), 1)
            plane = jnp.broadcast_to(below[:asked_rows], (asked_rows, HD))
            for k in heads[1:]:
                plane = jnp.where(
                    lane < k * part_lanes, plane, below[k * asked_rows : (k + 1) * asked_rows]
                )
            msg[dest, kv_local] = plane.astype(jnp.bfloat16).reshape(span * n_depth, block, HD)

        def finish(start):
            dest = pl.ds(start * n_depth, span * n_depth)
            both = [pltpu.matmul_pop(total[m]) for m in range(MXUS)]
            for k in heads:
                line, lanes = slice(k * asked_rows, (k + 1) * asked_rows), slice(k * HD, (k + 1) * HD)
                number = both[0][line, lanes]
                for m in range(1, MXUS):
                    number = number + both[m][line, lanes]
                msg[dest, k] = number.astype(jnp.bfloat16).reshape(span * n_depth, block, HD)

        def chunk_steps(c, chosen):
            return [together(t, chosen) for t in range(starts[c], starts[c] + CHUNKS[c])]

        def stage_scores(m, slot, key, ask):
            register = push(key, m, transpose=True)
            pltpu.matmul_acc_lhs(slot, ask, register)

        def stage_weights(j, slot, wanted, limits, first):
            lanes = weigh(j, slot, wanted, limits)
            if first:
                sums[...] = lanes
            else:
                sums[...] += lanes

        def stage_values(m, j, value):
            register = push(value, m)
            pltpu.matmul_acc_lhs(total[m], weighed[j], register)

        early, late = range(pairs), range(pairs, images)
        for c in range(final):
            end(chunk_copies(c))
            if c == 0:
                end(small)
            fetch(starts[c] + CHUNKS[c])
            project(chunk_steps(c, range(images)))
            if c == 0:
                prepare_queries()
            if c == MEET:
                pl.semaphore_wait(barrier, peers - 1)
                for offset in range(1, n_wide):
                    query_copy(offset).start()
        end(chunk_copies(final))
        half = CHUNKS[final] // 2
        if n_wide == span:

            def apart_steps(part, j):
                return [
                    apart(part, j, t, t + half) for t in range(starts[final], starts[final] + half)
                ]

            steps = []
            for j in early:
                steps += chunk_steps(final, [j])
            project(steps)
            for j in early:
                valued[j] = settle_values([accs[j][1]])
                keyed[j] = settle_keys([accs[j][0]])
            steps = []
            for j in late:
                steps += apart_steps(0, j)
            project(steps)
            read_queries()
            wanted, limits = wider(row_slot[...]), wider(row_limit[...])
            ask = asked(0)
            for n, (i, j) in enumerate(zip(early, late)):
                last_one = n + 1 == pairs
                slot = accs[j - pairs][1]
                stage_scores(0, accs[i][0], keyed[i], ask)
                if last_one:
                    stage_scores(1, slot, settle_keys([accs[j][0], slot]), ask)
                    project(apart_steps(1, j)[: half // 2])
                    for p in early[:-1]:
                        stage_weights(p, accs[p][0], wanted, limits, p == 0)
                        stage_values(0, p, valued[p])
                    project(apart_steps(1, j)[half // 2 :])
                else:
                    key = settle_keys([accs[j][0], slot])
                    project(apart_steps(1, j))
                    stage_scores(1, slot, key, ask)
            stage_weights(early[-1], accs[early[-1]][0], wanted, limits, pairs == 1)
            stage_values(0, early[-1], valued[early[-1]])
            for j in late:
                stage_weights(j, accs[j - pairs][1], wanted, limits, False)
                if j == late[-1]:
                    send_denominators(0)
                stage_values(1, j, settle_values(accs[j]))
            finish(0)
        else:
            project(chunk_steps(final, range(images)))
            read_queries()
            for j in range(images):
                keyed[j], valued[j] = settle_keys([accs[j][0]]), settle_values([accs[j][1]])

            def attend(s, carry):
                start = s * span
                here = pl.ds(start * group_rows, asked_rows)
                wanted, limits = wider(row_slot[here, :]), wider(row_limit[here, :])
                ask = asked(start)
                for j in range(images):
                    m, i = divmod(j, pairs)
                    pltpu.matmul_push_rhs(keyed[j], 0, m, transpose=True)
                    pltpu.matmul_acc_lhs(accs[i][m], ask, 0)
                for j in range(images):
                    m, i = divmod(j, pairs)
                    stage_weights(j, accs[i][m], wanted, limits, j == 0)
                for j in range(images):
                    m = j // pairs
                    pltpu.matmul_push_rhs(valued[j], 0, m)
                    pltpu.matmul_acc_lhs(total[m], weighed[j], 0)
                send_denominators(start)
                finish(start)
                return carry

            lax.fori_loop(0, n_wide // span, attend, 0)

    pl.run_scoped(
        run,
        *[
            pltpu.ACC(m)((rows, MXU), jnp.float32)
            for _ in range(images)
            for m in range(MXUS)
        ],
    )

    if peers <= 8:
        order = [
            a * n_depth + b
            for b in [*range(1, n_depth), 0]
            for a in [*range(1, n_wide), 0]
            if a or b
        ]
        for offset in order:
            result_copy(offset).start()
    else:

        def step(offset, carry):
            result_copy(offset).start()
            return carry

        lax.fori_loop(1, peers, step, 0)

    total = msg[me].astype(jnp.float32)
    all_results().wait_recv()

    def collect(offset, total):
        return total + got[offset - 1].astype(jnp.float32)

    total = lax.fori_loop(1, peers, collect, total, unroll=peers <= 8)
    for k in heads:
        res[...] = total[k] / total[kv_local, :, k * part_lanes : k * part_lanes + 1]
        for g in range(group):
            out[:, pl.ds((k * group + g) * HD, HD)] = res[pl.ds(g * share, share), :].astype(
                out.dtype
            )

    for offset in range(1, n_wide):
        query_copy(offset).wait_send()

    all_results().wait_send()


def local(
    n_wide,
    n_depth,
    patch_store,
    w_key,
    w_value,
    key_gain,
    query_gain,
    queries,
    owner_table,
    reader_table,
    request_image,
    image_tiles,
):
    images, rows, width = patch_store.shape
    kv_local = w_key.shape[1] // HD
    batch, q_cols = queries.shape
    group = q_cols // (kv_local * HD)
    share = batch // n_depth
    block = share * group
    group_rows = n_depth * block
    peers = n_wide * n_depth
    total_rows = peers * block
    anywhere = pl.BlockSpec(memory_space=pl.ANY)
    dma = pltpu.SemaphoreType.DMA
    return pl.pallas_call(
        functools.partial(kernel, n_wide, n_depth),
        out_shape=pltpu.VMEM((share, q_cols), jnp.bfloat16),
        in_specs=[anywhere] * 10,
        out_specs=pl.BlockSpec(memory_space=pltpu.VMEM),
        scratch_shapes=[
            pltpu.SMEM(owner_table.shape, jnp.int32),
            pltpu.SMEM(reader_table.shape, jnp.int32),
            pltpu.SMEM(request_image.shape, jnp.int32),
            pltpu.SMEM(image_tiles.shape, jnp.int32),
            pltpu.VMEM((images, rows, width), jnp.bfloat16),
            pltpu.VMEM((width, kv_local * HD), jnp.bfloat16),
            pltpu.VMEM((width, kv_local * HD), jnp.bfloat16),
            pltpu.VMEM((batch, q_cols), jnp.bfloat16),
            pltpu.VMEM((2, 1, HD), jnp.float32),
            pltpu.VMEM((batch, q_cols), jnp.float32),
            pltpu.VMEM((group_rows, HD), jnp.float32),
            pltpu.VMEM((n_wide, kv_local + 1, group_rows, HD), jnp.bfloat16),
            pltpu.VMEM((total_rows, HD), jnp.int32),
            pltpu.VMEM((total_rows, HD), jnp.int32),
            pltpu.VMEM((images, rows, kv_local * HD), jnp.bfloat16),
            pltpu.VMEM((images, rows, kv_local * HD), jnp.bfloat16),
            pltpu.VMEM((images, MXU, rows), jnp.bfloat16),
            pltpu.VMEM((MXU, HD), jnp.float32),
            pltpu.VMEM((peers, kv_local + 1, block, HD), jnp.bfloat16),
            pltpu.VMEM((peers - 1, kv_local + 1, block, HD), jnp.bfloat16),
            pltpu.VMEM((block, HD), jnp.float32),
            dma((len(CHUNKS),)),
            dma((1,)),
            dma((n_wide - 1,)),
            dma((n_wide - 1,)),
            dma((1,)),
            dma((1,)),
        ],
        compiler_params=pltpu.CompilerParams(
            collective_id=0, has_side_effects=True, vmem_limit_bytes=56 * 1024 * 1024
        ),
    )(
        patch_store,
        w_key,
        w_value,
        key_gain.reshape(1, HD),
        query_gain.reshape(1, HD),
        queries,
        owner_table,
        reader_table,
        request_image,
        image_tiles,
    )


def solution(mesh):
    placed = (
        P("wide", "depth", None),
        P(None, "narrow"),
        P(None, "narrow"),
        P(),
        P(),
        P("wide", "narrow"),
        P(),
        P(),
        P("wide"),
        P(),
    )
    return jax.shard_map(
        functools.partial(local, mesh.shape["wide"], mesh.shape["depth"]),
        mesh=mesh,
        in_specs=placed,
        out_specs=P(("wide", "depth"), "narrow"),
        check_vma=False,
    )
```

```python
import functools
import math

import jax
import jax.numpy as jnp
from jax import lax
from jax.experimental import pallas as pl
from jax.experimental.pallas import tpu as pltpu
from jax.sharding import PartitionSpec as P

HD = 128
TILE_P = 256
EPSILON = 1e-05
MXU = 256
MXUS = 2
CHUNKS = (2, 2, 4, 4, 4)
AHEAD = 8
MEET = 0
MESH = pl.DeviceIdType.MESH


def kernel(
    n_wide,
    n_depth,
    store,
    w_key,
    w_value,
    key_gain,
    query_gain,
    queries,
    owner_hbm,
    reader_hbm,
    request_hbm,
    tiles_hbm,
    out,
    owner_table,
    reader_table,
    request_image,
    image_tiles,
    xbuf,
    wkbuf,
    wvbuf,
    qraw,
    gains,
    qf,
    qs,
    qx,
    row_slot,
    row_limit,
    keyed,
    valued,
    weighed,
    sums,
    msg,
    got,
    res,
    c_sem,
    q_sem,
    q_send,
    q_recv,
    m_recv,
):
    images, rows, width = xbuf.shape
    kv_local = wkbuf.shape[1] // HD
    batch = qraw.shape[0]
    group = qraw.shape[1] // (kv_local * HD)
    share = batch // n_depth
    block = share * group
    group_rows = n_depth * block
    peers = n_wide * n_depth
    asked_rows = MXU // kv_local
    span = asked_rows // group_rows
    tiles = width // MXU
    pairs = images // MXUS
    wide, depth = lax.axis_index("wide"), lax.axis_index("depth")
    me = wide * n_depth + depth
    part_lanes = HD // kv_local
    heads = range(kv_local)

    barrier = pltpu.get_barrier_semaphore()

    def peer(offset):
        there = {
            "wide": lax.rem(wide + offset // n_depth, n_wide),
            "depth": lax.rem(depth + offset % n_depth, n_depth),
        }
        return there["wide"] * n_depth + there["depth"], there

    small = [
        pltpu.make_async_copy(queries, qraw, q_sem.at[0]),
        pltpu.make_async_copy(query_gain, gains.at[0], q_sem.at[0]),
        pltpu.make_async_copy(key_gain, gains.at[1], q_sem.at[0]),
        pltpu.make_async_copy(owner_hbm, owner_table, q_sem.at[0]),
        pltpu.make_async_copy(reader_hbm, reader_table, q_sem.at[0]),
        pltpu.make_async_copy(request_hbm, request_image, q_sem.at[0]),
        pltpu.make_async_copy(tiles_hbm, image_tiles, q_sem.at[0]),
    ]

    starts = [sum(CHUNKS[:c]) for c in range(len(CHUNKS))]

    final = len(CHUNKS) - 1

    def chunk_copies(c):
        piece = pl.ds(starts[c] * MXU, CHUNKS[c] * MXU)
        return [
            pltpu.make_async_copy(w_key.at[piece, :], wkbuf.at[piece, :], c_sem.at[c % 3]),
            pltpu.make_async_copy(store.at[:, :, piece], xbuf.at[:, :, piece], c_sem.at[c % 3]),
            pltpu.make_async_copy(
                w_value.at[piece, :], wvbuf.at[piece, :], c_sem.at[c % 3]
            ),
        ]

    def begin(copies):
        for copy in copies:
            copy.start()

    def end(copies):
        for copy in copies:
            copy.wait()

    begun = [0]

    def fetch(arrived):
        while begun[0] < len(CHUNKS):
            c = begun[0]
            if c and starts[c] + CHUNKS[c] > arrived + AHEAD:
                break
            begin(chunk_copies(c))
            if c == 0:
                begin(small)
            begun[0] += 1

    fetch(0)

    def greet(offset, carry):
        pl.semaphore_signal(barrier, inc=1, device_id=peer(offset)[1], device_id_type=MESH)
        return carry

    lax.fori_loop(1, peers, greet, 0, unroll=peers <= 8)

    def prepare_queries():
        gain = gains[0] * gains[1] * (1.0 / math.sqrt(HD))
        for h in range(kv_local * group):
            lanes = pl.ds(h * HD, HD)
            head = qraw[:, lanes].astype(jnp.float32)
            mean = jnp.mean(head * head, axis=-1, keepdims=True)
            qf[:, lanes] = head * lax.rsqrt(mean + EPSILON) * gain
        for k in heads:
            for t in range(n_depth):
                for g in range(group):
                    qs[pl.ds(t * block + g * share, share), :] = qf[
                        pl.ds(t * share, share), pl.ds((k * group + g) * HD, HD)
                    ]
            qx[wide, k] = qs[...].astype(jnp.bfloat16)
        row = lax.broadcasted_iota(jnp.int32, (group_rows, HD), 0)
        request = row // block * share + row % share
        entry = jnp.zeros((group_rows, HD), jnp.int32)
        for b in range(batch):
            entry = jnp.where(request == b, request_image[b], entry)
        qx[wide, kv_local] = entry.astype(jnp.float32).astype(jnp.bfloat16)

    def query_copy(offset):
        return pltpu.make_async_remote_copy(
            src_ref=qx.at[wide],
            dst_ref=qx.at[wide],
            send_sem=q_send.at[offset - 1],
            recv_sem=q_recv.at[offset - 1],
            device_id={"wide": lax.rem(wide + offset, n_wide)},
            device_id_type=MESH,
        )

    def query_landed(offset):
        source = lax.rem(wide + n_wide - offset, n_wide)
        return pltpu.make_async_remote_copy(
            src_ref=qx.at[source],
            dst_ref=qx.at[source],
            send_sem=q_send.at[offset - 1],
            recv_sem=q_recv.at[offset - 1],
            device_id={"wide": lax.rem(wide + offset, n_wide)},
            device_id_type=MESH,
        )

    def result_copy(offset):
        index, device = peer(offset)
        return pltpu.make_async_remote_copy(
            src_ref=msg.at[index],
            dst_ref=got.at[offset - 1],
            send_sem=q_sem.at[0],
            recv_sem=m_recv.at[0],
            device_id=device,
            device_id_type=MESH,
        )

    def all_results():
        every = pl.ds(0, peers - 1)
        return pltpu.make_async_remote_copy(
            src_ref=msg.at[every],
            dst_ref=got.at[every],
            send_sem=q_sem.at[0],
            recv_sem=m_recv.at[0],
            device_id=peer(1)[1],
            device_id_type=MESH,
        )

    whole_tiles = TILE_P % rows == 0

    def read_queries():
        for offset in range(1, n_wide):
            query_landed(offset).wait_recv()
        for g in range(n_wide):
            entry = qx[g, kv_local].astype(jnp.float32)
            slots = jnp.full((group_rows, HD), -1, jnp.int32)
            limits = jnp.zeros((group_rows, HD), jnp.int32)
            for r in range(reader_table.shape[1]):
                image = reader_table[g, r]
                slot = owner_table[image]
                limit = image_tiles[image] * TILE_P - depth * rows
                if whole_tiles:
                    slot = jnp.where(limit > 0, slot, -1)
                slots = jnp.where(entry == r, slot, slots)
                limits = jnp.where(entry == r, limit, limits)
            row_slot[pl.ds(g * group_rows, group_rows), :] = slots
            row_limit[pl.ds(g * group_rows, group_rows), :] = limits

    def wider(tile):
        return jnp.concatenate([tile] * (rows // HD), axis=1) if rows > HD else tile

    def run(*flat):
        accs = [flat[MXUS * j : MXUS * (j + 1)] for j in range(images)]
        total = [accs[0][0], accs[pairs][1]]
        turn = [0] * MXUS
        ready = []

        def push(tile, m, transpose=False):
            turn[m] ^= 1
            pltpu.matmul_push_rhs(tile, turn[m], m, transpose=transpose)
            return turn[m]

        def push_weights(step):
            ready.append(
                [
                    push((wkbuf, wvbuf)[part][pl.ds(t * MXU, MXU), :], m)
                    for m, (part, t) in enumerate(step[0])
                ]
            )

        def project(steps, after=None):
            if not ready:
                push_weights(steps[0])
            for n, (weights, rounds) in enumerate(steps):
                registers = ready.pop()
                for first, (j, slots) in enumerate(rounds):
                    patches = {}
                    for m, (part, t) in enumerate(weights):
                        if t not in patches:
                            patches[t] = xbuf[j, :, pl.ds(t * MXU, MXU)]
                        pltpu.matmul_acc_lhs(
                            slots[m], patches[t], None if first else registers[m]
                        )
                following = steps[n + 1] if n + 1 < len(steps) else after
                if following:
                    push_weights(following)

        def together(t, chosen):
            return [(0, t), (1, t)], [(j, accs[j]) for j in chosen]

        def apart(part, j, t, u):
            slots = [accs[j][0], accs[j - pairs if part == 0 else j][1]]
            return [(part, t), (part, u)], [(j, slots)]

        def popped(slots):
            return functools.reduce(jnp.add, [pltpu.matmul_pop(slot) for slot in slots])

        def settle_keys(slots):
            raw = popped(slots)
            done = []
            for k in heads:
                head = raw[:, k * HD : (k + 1) * HD]
                mean = jnp.mean(head * head, axis=-1, keepdims=True)
                done.append((head * lax.rsqrt(mean + EPSILON)).astype(jnp.bfloat16))
            return jnp.concatenate(done, axis=1)

        def settle_values(slots):
            return popped(slots).astype(jnp.bfloat16)

        def asked(start):
            lines = []
            for k in heads:
                ask = qx[pl.ds(start, span), k].reshape(asked_rows, HD)
                none = jnp.zeros_like(ask)
                lines.append(jnp.concatenate([ask if k == i else none for i in heads], axis=1))
            return jnp.concatenate(lines, axis=0)

        def weigh(j, slot, wanted, limits):
            scores = pltpu.matmul_pop(slot)
            keep = wanted == wide * images + j
            if not whole_tiles:
                place = lax.broadcasted_iota(jnp.int32, keep.shape, 1)
                keep = keep & (place < limits)
            keep = jnp.concatenate([keep] * kv_local, axis=0)
            weights = jnp.where(keep, jnp.exp(scores), 0.0)
            weighed[j] = weights.astype(jnp.bfloat16)
            lanes = weights[:, :HD]
            for at in range(HD, rows, HD):
                lanes = lanes + weights[:, at : at + HD]
            return lanes

        def send_denominators(start):
            dest = pl.ds(start * n_depth, span * n_depth)
            below = jnp.sum(sums[...], axis=-1, keepdims=True)
            lane = lax.broadcasted_iota(jnp.int32, (asked_rows, HD), 1)
            plane = jnp.broadcast_to(below[:asked_rows], (asked_rows, HD))
            for k in heads[1:]:
                plane = jnp.where(
                    lane < k * part_lanes, plane, below[k * asked_rows : (k + 1) * asked_rows]
                )
            msg[dest, kv_local] = plane.astype(jnp.bfloat16).reshape(span * n_depth, block, HD)

        def finish(start):
            dest = pl.ds(start * n_depth, span * n_depth)
            both = [pltpu.matmul_pop(total[m]) for m in range(MXUS)]
            for k in heads:
                line, lanes = slice(k * asked_rows, (k + 1) * asked_rows), slice(k * HD, (k + 1) * HD)
                number = both[0][line, lanes]
                for m in range(1, MXUS):
                    number = number + both[m][line, lanes]
                msg[dest, k] = number.astype(jnp.bfloat16).reshape(span * n_depth, block, HD)

        def chunk_steps(c, chosen):
            return [together(t, chosen) for t in range(starts[c], starts[c] + CHUNKS[c])]

        def stage_scores(m, slot, key, ask):
            register = push(key, m, transpose=True)
            pltpu.matmul_acc_lhs(slot, ask, register)

        def stage_weights(j, slot, wanted, limits, first):
            lanes = weigh(j, slot, wanted, limits)
            if first:
                sums[...] = lanes
            else:
                sums[...] += lanes

        def stage_values(m, j, value):
            register = push(value, m)
            pltpu.matmul_acc_lhs(total[m], weighed[j], register)

        early, late = range(pairs), range(pairs, images)
        for c in range(final):
            end(chunk_copies(c))
            if c == 0:
                end(small)
            fetch(starts[c] + CHUNKS[c])
            project(chunk_steps(c, range(images)))
            if c == 0:
                prepare_queries()
            if c == MEET:
                pl.semaphore_wait(barrier, peers - 1)
                for offset in range(1, n_wide):
                    query_copy(offset).start()
        end(chunk_copies(final))
        half = CHUNKS[final] // 2
        if n_wide == span:

            def apart_steps(part, j):
                return [
                    apart(part, j, t, t + half) for t in range(starts[final], starts[final] + half)
                ]

            steps = []
            for j in early:
                steps += chunk_steps(final, [j])
            project(steps)
            for j in early:
                valued[j] = settle_values([accs[j][1]])
                keyed[j] = settle_keys([accs[j][0]])
            steps = []
            for j in late:
                steps += apart_steps(0, j)
            project(steps)
            read_queries()
            wanted, limits = wider(row_slot[...]), wider(row_limit[...])
            ask = asked(0)
            for n, (i, j) in enumerate(zip(early, late)):
                last_one = n + 1 == pairs
                slot = accs[j - pairs][1]
                stage_scores(0, accs[i][0], keyed[i], ask)
                if last_one:
                    stage_scores(1, slot, settle_keys([accs[j][0], slot]), ask)
                    project(apart_steps(1, j)[: half // 2])
                    for p in early[:-1]:
                        stage_weights(p, accs[p][0], wanted, limits, p == 0)
                        stage_values(0, p, valued[p])
                    project(apart_steps(1, j)[half // 2 :])
                else:
                    key = settle_keys([accs[j][0], slot])
                    project(apart_steps(1, j))
                    stage_scores(1, slot, key, ask)
            stage_weights(early[-1], accs[early[-1]][0], wanted, limits, pairs == 1)
            stage_values(0, early[-1], valued[early[-1]])
            for j in late:
                stage_weights(j, accs[j - pairs][1], wanted, limits, False)
                if j == late[-1]:
                    send_denominators(0)
                stage_values(1, j, settle_values(accs[j]))
            finish(0)
        else:
            project(chunk_steps(final, range(images)))
            read_queries()
            for j in range(images):
                keyed[j], valued[j] = settle_keys([accs[j][0]]), settle_values([accs[j][1]])

            def attend(s, carry):
                start = s * span
                here = pl.ds(start * group_rows, asked_rows)
                wanted, limits = wider(row_slot[here, :]), wider(row_limit[here, :])
                ask = asked(start)
                for j in range(images):
                    m, i = divmod(j, pairs)
                    pltpu.matmul_push_rhs(keyed[j], 0, m, transpose=True)
                    pltpu.matmul_acc_lhs(accs[i][m], ask, 0)
                for j in range(images):
                    m, i = divmod(j, pairs)
                    stage_weights(j, accs[i][m], wanted, limits, j == 0)
                for j in range(images):
                    m = j // pairs
                    pltpu.matmul_push_rhs(valued[j], 0, m)
                    pltpu.matmul_acc_lhs(total[m], weighed[j], 0)
                send_denominators(start)
                finish(start)
                return carry

            lax.fori_loop(0, n_wide // span, attend, 0)

    pl.run_scoped(
        run,
        *[
            pltpu.ACC(m)((rows, MXU), jnp.float32)
            for _ in range(images)
            for m in range(MXUS)
        ],
    )

    if peers <= 8:
        order = [
            a * n_depth + b
            for b in [*range(1, n_depth), 0]
            for a in [*range(1, n_wide), 0]
            if a or b
        ]
        for offset in order:
            result_copy(offset).start()
    else:

        def step(offset, carry):
            result_copy(offset).start()
            return carry

        lax.fori_loop(1, peers, step, 0)

    total = msg[me].astype(jnp.float32)
    all_results().wait_recv()

    def collect(offset, total):
        return total + got[offset - 1].astype(jnp.float32)

    total = lax.fori_loop(1, peers, collect, total, unroll=peers <= 8)
    for k in heads:
        res[...] = total[k] / total[kv_local, :, k * part_lanes : k * part_lanes + 1]
        for g in range(group):
            out[:, pl.ds((k * group + g) * HD, HD)] = res[pl.ds(g * share, share), :].astype(
                out.dtype
            )

    for offset in range(1, n_wide):
        query_copy(offset).wait_send()

    all_results().wait_send()


def local(
    n_wide,
    n_depth,
    patch_store,
    w_key,
    w_value,
    key_gain,
    query_gain,
    queries,
    owner_table,
    reader_table,
    request_image,
    image_tiles,
):
    images, rows, width = patch_store.shape
    kv_local = w_key.shape[1] // HD
    batch, q_cols = queries.shape
    group = q_cols // (kv_local * HD)
    share = batch // n_depth
    block = share * group
    group_rows = n_depth * block
    peers = n_wide * n_depth
    total_rows = peers * block
    anywhere = pl.BlockSpec(memory_space=pl.ANY)
    dma = pltpu.SemaphoreType.DMA
    return pl.pallas_call(
        functools.partial(kernel, n_wide, n_depth),
        out_shape=pltpu.VMEM((share, q_cols), jnp.bfloat16),
        in_specs=[anywhere] * 10,
        out_specs=pl.BlockSpec(memory_space=pltpu.VMEM),
        scratch_shapes=[
            pltpu.SMEM(owner_table.shape, jnp.int32),
            pltpu.SMEM(reader_table.shape, jnp.int32),
            pltpu.SMEM(request_image.shape, jnp.int32),
            pltpu.SMEM(image_tiles.shape, jnp.int32),
            pltpu.VMEM((images, rows, width), jnp.bfloat16),
            pltpu.VMEM((width, kv_local * HD), jnp.bfloat16),
            pltpu.VMEM((width, kv_local * HD), jnp.bfloat16),
            pltpu.VMEM((batch, q_cols), jnp.bfloat16),
            pltpu.VMEM((2, 1, HD), jnp.float32),
            pltpu.VMEM((batch, q_cols), jnp.float32),
            pltpu.VMEM((group_rows, HD), jnp.float32),
            pltpu.VMEM((n_wide, kv_local + 1, group_rows, HD), jnp.bfloat16),
            pltpu.VMEM((total_rows, HD), jnp.int32),
            pltpu.VMEM((total_rows, HD), jnp.int32),
            pltpu.VMEM((images, rows, kv_local * HD), jnp.bfloat16),
            pltpu.VMEM((images, rows, kv_local * HD), jnp.bfloat16),
            pltpu.VMEM((images, MXU, rows), jnp.bfloat16),
            pltpu.VMEM((MXU, HD), jnp.float32),
            pltpu.VMEM((peers, kv_local + 1, block, HD), jnp.bfloat16),
            pltpu.VMEM((peers - 1, kv_local + 1, block, HD), jnp.bfloat16),
            pltpu.VMEM((block, HD), jnp.float32),
            dma((3,)),
            dma((1,)),
            dma((n_wide - 1,)),
            dma((n_wide - 1,)),
            dma((1,)),
        ],
        compiler_params=pltpu.CompilerParams(
            collective_id=0, has_side_effects=True, vmem_limit_bytes=56 * 1024 * 1024
        ),
    )(
        patch_store,
        w_key,
        w_value,
        key_gain.reshape(1, HD),
        query_gain.reshape(1, HD),
        queries,
        owner_table,
        reader_table,
        request_image,
        image_tiles,
    )


def solution(mesh):
    placed = (
        P("wide", "depth", None),
        P(None, "narrow"),
        P(None, "narrow"),
        P(),
        P(),
        P("wide", "narrow"),
        P(),
        P(),
        P("wide"),
        P(),
    )
    return jax.shard_map(
        functools.partial(local, mesh.shape["wide"], mesh.shape["depth"]),
        mesh=mesh,
        in_specs=placed,
        out_specs=P(("wide", "depth"), "narrow"),
        check_vma=False,
    )
```
